256 devices in a mesh: ep: 64 (over x, z, core), dp: 4 (over y).
Axes of the slice: x: 4, y: 4, z: 8, core: 2. Of those that a mesh axis runs over, the one named last changes fastest.
Arguments:
- tokens: bfloat16 [32768, 2048], P(('ep', 'dp')), may hold values from -6 to 6
- routes: int32 [32768, 8], P(('ep', 'dp')), may hold values from 0 to 63, as said below
- gates: bfloat16 [32768, 8], P(('ep', 'dp')), may hold values from 0.19921875 to 1
- w_gate: bfloat16 [64, 2048, 768], P('ep'), may hold values from -0.125 to 0.125
- w_up: bfloat16 [64, 2048, 768], P('ep'), may hold values from -0.125 to 0.125
- w_down: bfloat16 [64, 768, 2048], P('ep'), may hold values from -0.21875 to 0.21875
- score_head: float32 [2048], replicated, may hold values from -0.125 to 0.125
- doc_ids: int32 [256], P(('ep', 'dp')), may hold values from 0 to 63, never falling along the last dimension, each value on 1 to 8 neighbouring positions
Outputs:
- mixed: bfloat16 [32768, 2048], P(('ep', 'dp'))
- doc_scores: float32 [3, 64], replicated
The draws below stay inside these ranges and needn't reach their ends.
Inputs may be any that keep to these rules, and one draw needn't show every extreme that they name: `routes`: each row names 8 different experts; among the rows of one device no expert is named more than 24 times. `doc_ids`: never falling along the passages; every document has 1 to 8 passages.
All inputs are finite; a program needn't handle non-finite values.
Results may differ from the reference program's by a relative error of at most 0.0058.
Values may be sent and summed in bfloat16 or wider, within the bound.
A program may use at most 64 MiB of HBM per device.

```python
import math
import jax
import jax.numpy as jnp
import numpy as np
from jax import lax

D = 2048
FF = 768
TOP = 8
PASSAGE = 128
DOC_MOST = 8
TOK_DEV = 128
EXPERTS = 64
CAP = 24
TOKENS = 32768
PASSAGES = 256
DOCS = 64
N_EP = 64
N_DP = 4


def route_block(block_key, hot):
    row_pos = jnp.arange(TOK_DEV, dtype=jnp.int32)[:, None]
    column_pos = jnp.arange(TOP, dtype=jnp.int32)[None, :]
    lower = jnp.where(column_pos == 0, -1, row_pos * (TOP - 1) + column_pos - 1)
    upper = CAP * (TOP - 1) + (row_pos - CAP) * TOP + column_pos
    position = jnp.where(row_pos < CAP, lower, upper).astype(jnp.int32)
    others = jax.random.permutation(jax.random.fold_in(block_key, 1), EXPERTS - 1).astype(jnp.int32)
    listed = (others + (others >= hot).astype(jnp.int32)).astype(jnp.int32)
    picks = listed[jnp.maximum(position, 0) % (EXPERTS - 1)]
    picks = jnp.where(position < 0, hot, picks).astype(jnp.int32)
    row_order = jax.random.permutation(jax.random.fold_in(block_key, 2), TOK_DEV).astype(jnp.int32)
    picks = picks[row_order]
    column_keys = jax.random.split(jax.random.fold_in(block_key, 3), TOK_DEV)
    column_order = jax.vmap(lambda one_key: jax.random.permutation(one_key, TOP))(column_keys).astype(jnp.int32)
    return jnp.take_along_axis(picks, column_order, axis=1).astype(jnp.int32)


def draw_routes(key, part):
    block_count = TOKENS // TOK_DEV
    first_hot = jax.random.randint(jax.random.fold_in(key, 11), (), 0, EXPERTS).astype(jnp.int32)
    block_index = jnp.arange(block_count, dtype=jnp.int32)
    group = block_index % N_DP
    hot_list = ((first_hot + group * (EXPERTS // N_DP)) % EXPERTS).astype(jnp.int32)
    block_keys = jax.vmap(lambda index: jax.random.fold_in(jax.random.fold_in(key, 17), index))(block_index)
    blocks = jax.vmap(route_block)(block_keys, hot_list)
    return blocks.reshape(TOKENS, TOP).astype(jnp.int32)


def levels(rng, extent, pieces, least, high):
    def one(dim, blocks):
        draws = jax.random.uniform(jax.random.fold_in(jax.random.fold_in(rng, 6), dim), (blocks,), jnp.float32, least / len(pieces), high / len(pieces))
        return jnp.repeat(jnp.exp(draws), extent[dim] // blocks).reshape((-1,) + (1,) * (len(extent) - dim - 1))

    factor_of = one(*pieces[0])
    for cut in pieces[1:]:
        factor_of = factor_of * one(*cut)
    return factor_of


def profile(amount, total, most, skew):
    weights = [(1 << 20) // math.isqrt(rank ** skew) + 1 for rank in range(2, amount + 1)]
    rest, counts = total - most - (amount - 1), [1] * (amount - 1)
    while rest > 0:
        candidates = [i for i in range(amount - 1) if counts[i] < most]
        pool, left = sum([weights[i] for i in candidates]), rest
        for i in candidates:
            more = min(most - counts[i], max(1, left * weights[i] // pool), rest)
            counts[i] = counts[i] + more
            rest = rest - more
    return np.array([most] + counts)


def ragged(rng, amount, total, reach, skew):
    if amount == 2:
        one = jax.random.randint(rng, (), max(1, total - reach), min(reach, total - 1) + 1)
        return jnp.stack([one, total - one])
    tallies = jnp.asarray(profile(amount, total, reach, skew), jnp.int32)
    couples = (amount - 1) // 2
    source_of, sink = tallies[1:1 + 2 * couples:2], tallies[2:2 + 2 * couples:2]
    slack = jnp.minimum(source_of - 1, reach - sink)
    shifted = jax.random.randint(jax.random.fold_in(rng, 1), (couples,), 0, 1 << 20) % (slack + 1)
    tallies = tallies.at[1:1 + 2 * couples:2].set(source_of - shifted).at[2:2 + 2 * couples:2].set(sink + shifted)
    return tallies[jax.random.permutation(jax.random.fold_in(rng, 2), amount)]


def noise(stream_key, dims, spread, most, cuts=(), held_as=jnp.bfloat16):
    array = jax.random.normal(stream_key, dims, jnp.float32) * spread
    if len(cuts) > 0:
        array = levels(stream_key, dims, cuts, -0.22, 0.18) * array
    return jnp.clip(array, min=-most, max=most).astype(held_as)


def setup_inputs(seed: int = 0) -> dict:
    arg_keys = jax.random.split(jax.random.key(seed), 9)
    return {
        "tokens": noise(arg_keys[0], (TOKENS, D), 1.0, 6.0, ((0, 256),)),
        "routes": draw_routes(jax.random.fold_in(arg_keys[8], 71), 0),
        "gates": jnp.clip(jnp.exp(math.log(1.0) - 1.6133518 * jax.random.uniform(arg_keys[2], (TOKENS, TOP), jnp.float32) ** levels(arg_keys[2], (TOKENS, TOP), ((0, 256),), -0.2, 0.2)), 0.19921875, 1.0).astype(jnp.bfloat16),
        "w_gate": noise(arg_keys[3], (EXPERTS, D, FF), D ** -0.5, 0.125, ((0, 64),)),
        "w_up": noise(arg_keys[4], (EXPERTS, D, FF), D ** -0.5, 0.125, ((0, 64),)),
        "w_down": noise(arg_keys[5], (EXPERTS, FF, D), FF ** -0.5, 0.21875, ((0, 64),)),
        "score_head": noise(arg_keys[6], (D,), D ** -0.5, 0.125, (), jnp.float32),
        "doc_ids": jnp.searchsorted(jnp.cumsum(ragged(arg_keys[7], DOCS, PASSAGES, DOC_MOST, 2)), jnp.arange(PASSAGES), side="right").astype(jnp.int32),
    }


block_rows = 256

def expert_rows(rows, gate_rows, wg_single, wu_single, wd_single):
    gate_part = jnp.dot(rows, wg_single, preferred_element_type=jnp.float32)
    up_part = jnp.dot(rows, wu_single, preferred_element_type=jnp.float32)
    hidden = (jax.nn.silu(gate_part) * up_part).astype(jnp.bfloat16)
    result = jnp.dot(hidden, wd_single, preferred_element_type=jnp.float32)
    return (gate_rows.astype(jnp.float32)[:, None] * result).astype(jnp.bfloat16)

def reference(tokens, routes, gates, w_gate, w_up, w_down, score_head, doc_ids):
    flat_routes = routes.reshape(-1)
    flat_gates = gates.reshape(-1)
    span = -(-(CAP * N_EP * N_DP) // block_rows) * block_rows

    def per_expert(total, expert):
        chosen_mask = flat_routes == expert
        live_count = jnp.sum(chosen_mask.astype(jnp.int32))
        chosen = jnp.nonzero(chosen_mask, size=span, fill_value=0)[0].astype(jnp.int32)
        wg_single = w_gate[expert]
        wu_single = w_up[expert]
        wd_single = w_down[expert]

        def keep_going(state):
            return state[0] * block_rows < live_count

        def one_block(state):
            block_index, running = state
            pair_index = lax.dynamic_slice_in_dim(chosen, block_index * block_rows, block_rows)
            valid = block_index * block_rows + jnp.arange(block_rows, dtype=jnp.int32) < live_count
            token_index = (pair_index // TOP).astype(jnp.int32)
            weighted = expert_rows(tokens[token_index], flat_gates[pair_index], wg_single, wu_single, wd_single)
            addend = jnp.where(valid[:, None], weighted.astype(jnp.float32), jnp.float32(0.0))
            return (block_index + 1, running.at[token_index].add(addend))
        _, total = lax.while_loop(keep_going, one_block, (jnp.int32(0), total))
        return (total, None)
    start_total = jnp.zeros((TOKENS, D), jnp.float32)
    total, _ = lax.scan(per_expert, start_total, jnp.arange(EXPERTS, dtype=jnp.int32))
    mixed = total.astype(jnp.bfloat16)
    token_score = jnp.dot(mixed.astype(jnp.float32), score_head, precision=lax.Precision.HIGHEST)
    passage_score = token_score.reshape(-1, PASSAGE).sum(axis=1) / math.sqrt(PASSAGE)
    member = doc_ids[:, None] == jnp.arange(DOCS, dtype=jnp.int32)[None, :]
    column = passage_score[:, None]
    max_score = jnp.where(member, column, -1e+30).max(axis=0)
    sum_score = jnp.where(member, column, 0.0).sum(axis=0)
    passage_index = jnp.arange(PASSAGES, dtype=jnp.int32)[:, None]
    first_index = jnp.where(member, passage_index, PASSAGES).min(axis=0)
    first_score = jnp.where(member & (passage_index == first_index[None, :]), column, 0.0).sum(axis=0)
    return (mixed, jnp.stack([max_score, first_score, sum_score]))
```

```python
import math

import jax
import jax.numpy as jnp
from jax import lax
from jax.sharding import Mesh
from jax.sharding import PartitionSpec as P

TOP = 8
PASSAGE = 128
EP = ("x", "z", "core")
EP_DP = ("x", "z", "core", "dp")
CAP = 24


def shards(tokens, routes, gates, w_gate, w_up, w_down, score_head, doc_ids):
    rows, width = tokens.shape
    nx, nz, nc = lax.axis_size("x"), lax.axis_size("z"), lax.axis_size("core")
    experts = nx * nz * nc
    hit = routes[:, :, None] == jnp.arange(experts, dtype=jnp.int32)
    routed = hit.any(axis=1)
    gate_of = jnp.where(hit, gates[:, :, None], 0).sum(axis=1)
    below = jnp.tril(jnp.ones((rows, rows), jnp.bfloat16), -1)
    rank = jnp.dot(below, routed.astype(jnp.bfloat16), preferred_element_type=jnp.float32)
    rank = jnp.where(routed, rank, 200.0).astype(jnp.bfloat16)
    packed = jnp.concatenate([tokens, rank, gate_of.astype(jnp.bfloat16)], axis=1)
    held = lax.all_gather(packed, "z")
    mine = lax.axis_index("z")

    def at_z(a):
        a = a.reshape(nz, rows, nx, nz, nc)
        return lax.dynamic_index_in_dim(a, mine, 3, keepdims=False).reshape(nz, rows, nx * nc)

    rank_z = at_z(held[..., width : width + experts])
    gate_z = at_z(held[..., width + experts :])
    slots = jnp.arange(CAP, dtype=jnp.bfloat16)
    chosen = rank_z.transpose(2, 0, 1)[:, :, None, :] == slots[:, None]
    pick = chosen.astype(jnp.bfloat16)
    send = jnp.einsum("dslt,stf->dslf", pick, held[..., :width], preferred_element_type=jnp.bfloat16)
    send = send.reshape(nx * nc, nz * CAP, width)
    recv = lax.all_to_all(send, ("x", "core"), split_axis=0, concat_axis=0, tiled=True)
    flat = recv.reshape(-1, width)
    gate_part = jnp.dot(flat, w_gate[0], preferred_element_type=jnp.float32)
    up_part = jnp.dot(flat, w_up[0], preferred_element_type=jnp.float32)
    hidden = (jax.nn.silu(gate_part) * up_part).astype(jnp.bfloat16)
    result = jnp.dot(hidden, w_down[0], preferred_element_type=jnp.float32).astype(jnp.bfloat16)
    back = lax.all_to_all(
        result.reshape(recv.shape), ("x", "core"), split_axis=0, concat_axis=0, tiled=True
    ).reshape(nx * nc, nz, CAP, width)
    mix = jnp.where(chosen, gate_z.transpose(2, 0, 1)[:, :, None, :], 0)
    part = jnp.einsum("dslt,dslf->stf", mix, back, preferred_element_type=jnp.float32)
    mixed = lax.psum_scatter(part.astype(jnp.bfloat16), "z", scatter_dimension=0, tiled=False)

    token_score = jnp.dot(mixed.astype(jnp.float32), score_head, precision=lax.Precision.HIGHEST)
    passage_score = token_score.reshape(-1, PASSAGE).sum(axis=1) / math.sqrt(PASSAGE)
    pair = jnp.stack([passage_score, doc_ids.astype(jnp.float32)], axis=1)
    pairs = lax.all_gather(pair, EP_DP, tiled=True)
    total = pairs.shape[0]
    docs = total // 4
    column = pairs[:, :1]
    member = pairs[:, 1:] == jnp.arange(docs, dtype=jnp.float32)[None, :]
    index = jnp.arange(total, dtype=jnp.int32)[:, None]
    max_score = jnp.where(member, column, -1e30).max(axis=0)
    sum_score = jnp.where(member, column, 0.0).sum(axis=0)
    first = jnp.where(member, index, total).min(axis=0)
    first_score = jnp.where(member & (index == first[None, :]), column, 0.0).sum(axis=0)
    return mixed, jnp.stack([max_score, first_score, sum_score])


def solution(mesh):
    finer = Mesh(mesh.devices.reshape(4, 8, 2, mesh.shape["dp"]), EP_DP)
    return jax.shard_map(
        shards,
        mesh=finer,
        in_specs=(
            P(EP_DP, None),
            P(EP_DP, None),
            P(EP_DP, None),
            P(EP, None, None),
            P(EP, None, None),
            P(EP, None, None),
            P(),
            P(EP_DP),
        ),
        out_specs=(P(EP_DP, None), P()),
        check_vma=False,
    )
```
